32 devices in a mesh: dp: 4 (over y, x), vocab: 8 (over z, core).
Axes of the slice: x: 2, y: 2, z: 4, core: 2. Of those that a mesh axis runs over, the one named last changes fastest.
Arguments:
- hidden: bfloat16 [2048, 5120], P(('dp', 'vocab')), may hold values from -100 to 100
- tokens: int32 [2048], P('dp'), may hold values from 0 to 9215
- old_weight: bfloat16 [9216, 5120], P('vocab'), may hold values from -1 to 1
- new_weight: bfloat16 [9216, 5120], P('dp', 'vocab'), may hold values from -6 to 6
Outputs:
- logprob: float32 [2048], P(('dp', 'vocab'))
- engine_weight: bfloat16 [9216, 5120], P('vocab')
The draws below stay inside these ranges and needn't reach their ends.
All inputs are finite; a program needn't handle non-finite values.
Results may differ from the reference program's by a relative error of at most 0.001.
Values may be sent and summed in bfloat16 or wider, within the bound.
A program may use at most 128 MiB of HBM per device.

```python
import math
import jax
import jax.numpy as jnp
from jax import lax

D = 5120
VOCAB = 9216
GROUP_ROWS = 512
ROWS = 2048
N_DP = 4


def base_weight(key):
    first_key = jax.random.fold_in(jax.random.fold_in(key, 11), 0)
    weights = jax.random.normal(first_key, (VOCAB, D), jnp.float32) / math.sqrt(D)
    return jnp.clip(weights, -1.0, 1.0)


def draw_old_weight(key, part):
    return base_weight(key).astype(jnp.bfloat16)


def draw_hidden(key, part):
    keys = jax.random.split(jax.random.fold_in(key, 23), 1)
    values = 3.0 * jax.random.normal(keys[0], (ROWS, D), jnp.float32)
    return jnp.clip(values, -100.0, 100.0).astype(jnp.bfloat16)


def set_ends(array, own_key, smallest, high):
    spot = [jax.random.randint(jax.random.fold_in(own_key, axis), (), 0, length) for axis, length in enumerate(array.shape)]
    longest = array.shape.index(max(array.shape))
    neighbour = spot[:longest] + [(spot[longest] + 1) % array.shape[longest]] + spot[longest + 1:]
    return array.at[tuple(spot)].set(smallest).at[tuple(neighbour)].set(high)


def levels(stream_key, shape, shards, least, top_value):
    gain = 1.0
    for position, shards_of in shards:
        steps = jax.random.uniform(jax.random.fold_in(jax.random.fold_in(stream_key, 6), position), (shards_of,), jnp.float32, least / len(shards), top_value / len(shards))
        gain = gain * jnp.repeat(jnp.exp(steps), shape[position] // shards_of).reshape((-1,) + (1,) * (len(shape) - 1 - position))
    return gain


def bell_draw(key, shape, deviation, bound, shards=(), dtype=jnp.bfloat16):
    result = deviation * jax.random.normal(key, shape, jnp.float32)
    if shards:
        result = result * levels(key, shape, shards, -0.22, 0.18)
    return jnp.clip(result, -bound, bound).astype(dtype)


def setup_inputs(seed: int = 0) -> dict:
    key_of = jax.random.split(jax.random.key(seed), 5)
    hidden = draw_hidden(jax.random.fold_in(key_of[4], 71), 0)
    tokens = set_ends(jax.random.randint(key_of[1], (ROWS,), 0, VOCAB), jax.random.fold_in(key_of[1], 1), 0, VOCAB - 1).astype(jnp.int32)
    old_weight = draw_old_weight(jax.random.fold_in(key_of[4], 71), 0)
    new_weight = bell_draw(key_of[3], (VOCAB, D), 1.0, 6.0, ((0, 4), (1, 8)))
    return dict(hidden=hidden, tokens=tokens, old_weight=old_weight, new_weight=new_weight)


def reference(hidden, tokens, old_weight, new_weight):
    def one_group(operands):
        rows, ids = operands
        logits = jnp.dot(rows, old_weight.T, preferred_element_type=jnp.float32)
        top = jnp.max(logits, axis=1)
        total = jnp.sum(jnp.exp(logits - top[:, None]), axis=1)
        target = jnp.take_along_axis(logits, ids[:, None].astype(jnp.int32), axis=1)[:, 0]
        return target - top - jnp.log(total)

    grouped = hidden.reshape(N_DP, GROUP_ROWS, D)
    grouped_ids = tokens.reshape(N_DP, GROUP_ROWS)
    logprob = lax.map(one_group, (grouped, grouped_ids)).reshape(ROWS)
    return logprob, new_weight
```

```python
import functools

import jax
import jax.numpy as jnp
from jax import lax
from jax.experimental import pallas as pl
from jax.experimental.pallas import tpu as pltpu
from jax.sharding import PartitionSpec as P

MESH = pl.DeviceIdType.MESH
STRIPE = 384


def pick(index, choices):
    value = jnp.int32(choices[0])
    for k in range(1, len(choices)):
        value = jnp.where(index == k, choices[k], value)
    return value


def nearest_first(count):
    return [sorted(range(count), key=lambda other: (abs(other - own), other)) for own in range(count)]


def exchange(
    replicas, ranks, tokens, hidden, old, new, pieces, logprob,
    gathered, weight, logits, stats, local_sem, weight_sem,
    line_send, line_recv, pair_send, pair_recv,
    spread_send, spread_recv, cube_send, cube_recv, stat_send, stat_recv,
):
    d = lax.axis_index("dp")
    v = lax.axis_index("vocab")
    owners = ranks // replicas
    groups = ranks // 2
    g, core = v // 2, v % 2
    own_rows = hidden.shape[0]
    vocab_rows = old.shape[0]
    part = vocab_rows // replicas
    half = (part // 2) // 16 * 16
    bits = replicas.bit_length() - 1

    def remote(src, dst, send, recv, device):
        return pltpu.make_async_remote_copy(
            src_ref=src, dst_ref=dst, send_sem=send, recv_sem=recv, device_id=device, device_id_type=MESH
        )

    def rows_of(rank):
        return gathered.at[pl.ds(pl.multiple_of(rank * own_rows, own_rows), own_rows), :]

    def line(group, step, source=None):
        slot = rows_of(2 * group + core)
        way = 0 if step > 0 else 1
        return remote(
            slot if source is None else source, slot, line_send.at[way, group], line_recv.at[way, group],
            (d, v + 2 * step),
        )

    def pair(group, source=None):
        slot = rows_of(2 * group + core)
        return remote(
            slot if source is None else source, slot, pair_send.at[group], pair_recv.at[group], (d, v + 1 - 2 * core)
        )

    def pair_arrival(group):
        slot = rows_of(2 * group + 1 - core)
        return remote(slot, slot, pair_send.at[group], pair_recv.at[group], (d, v + 1 - 2 * core))

    own_copy = pltpu.make_async_copy(hidden, rows_of(v), local_sem.at[0])
    own_copy.start()
    pl.when(g < groups - 1)(lambda: line(g, 1, hidden).start())
    pl.when(g > 0)(lambda: line(g, -1, hidden).start())
    pair(g, hidden).start()

    def line_step(step):
        def below():
            line(g - step, 1).wait_recv()
            pl.when(g < groups - 1)(lambda: line(g - step, 1).start())
            pair(g - step).start()

        def above():
            line(g + step, -1).wait_recv()
            pl.when(g > 0)(lambda: line(g + step, -1).start())
            pair(g + step).start()

        pl.when(g >= step)(below)
        pl.when(g + step < groups)(above)

    def spread(offset, owner, stay=False):
        target = d ^ offset
        source = new.at[pl.ds(pl.multiple_of(owner * vocab_rows + target * part, 16), part), :]
        slot = pieces.at[v, pl.ds(pl.multiple_of(target * part, 16), part), :]
        if stay:
            return pltpu.make_async_copy(source, slot, spread_recv.at[v])
        index = offset * owners + owner
        return remote(source, slot, spread_send.at[index], spread_recv.at[v], (target, d * owners + owner))

    def spread_start(offset, owner):
        if offset:
            spread(offset, owner).start()
        else:
            pl.when(d * owners + owner == v)(lambda: spread(offset, owner, stay=True).start())
            pl.when(d * owners + owner != v)(lambda: spread(offset, owner).start())

    def spread_sent(offset, owner):
        if offset:
            spread(offset, owner).wait_send()
        else:
            pl.when(d * owners + owner != v)(lambda: spread(offset, owner).wait_send())

    def spread_arrival(source):
        slot = pieces.at[source, pl.ds(pl.multiple_of(d * part, 16), part), :]
        pltpu.make_async_copy(slot, slot, spread_recv.at[source]).wait()

    def span(holder, which):
        first, length = {"all": (0, part), "low": (0, half), "high": (half, part - half)}[which]
        return pl.ds(pl.multiple_of(holder * part + first, 16), length)

    links = []
    for mask in range(replicas):
        for bit in range(bits):
            if mask >> bit & 1:
                continue
            if mask == 0:
                links.append((mask, bit, "all"))
                continue
            if bit > mask.bit_length() - 1:
                links.append((mask, bit, "low"))
            if bit < (mask & -mask).bit_length() - 1:
                links.append((mask, bit, "high"))

    def cube(source, index):
        mask, bit, which = links[index]
        slot = pieces.at[source, span(d ^ mask, which), :]
        return remote(slot, slot, cube_send.at[source, index], cube_recv.at[source, index], (d ^ (1 << bit), v))

    def cube_arrival(source, index):
        mask, bit, which = links[index]
        slot = pieces.at[source, span(d ^ mask ^ (1 << bit), which), :]
        remote(slot, slot, cube_send.at[source, index], cube_recv.at[source, index], (d ^ (1 << bit), v)).wait_recv()

    def cube_level(source, level):
        for index, (mask, bit, which) in enumerate(links):
            if mask.bit_count() == level - 1:
                cube_arrival(source, index)
                for onward, (held, _, wanted) in enumerate(links):
                    if held == mask | 1 << bit and which in ("all", wanted):
                        cube(source, onward).start()

    for offset in list(range(1, replicas)) + [0]:
        for owner in range(owners):
            spread_start(offset, owner)

    weight_copy = pltpu.make_async_copy(old, weight, weight_sem.at[0])
    weight_copy.start()

    table = nearest_first(groups)

    def sources(step):
        group = pick(g, [table[own][step] for own in range(groups)])
        return [2 * group, 2 * group + 1]

    def first_level(step):
        for source in sources(step):
            spread_arrival(source)
            for index, (mask, _, _) in enumerate(links):
                if mask == 0:
                    cube(source, index).start()

    def later_levels(step):
        for level in range(1, bits + 1):
            for source in sources(step):
                cube_level(source, level)

    def matmul():
        for group in range(groups):
            pair_arrival(group).wait_recv()
        own_copy.wait()
        weight_copy.wait()
        wanted = tokens[...] - v * vocab_rows
        count = gathered.shape[0]

        def stripe(index, carry):
            top, total, target = carry
            first = pl.multiple_of(index * STRIPE, STRIPE)
            logits[...] = lax.dot_general(
                weight[pl.ds(first, STRIPE), :], gathered[...], (((1,), (1,)), ((), ())),
                preferred_element_type=jnp.float32,
            )
            values = logits[...]
            higher = jnp.maximum(top, jnp.max(values, axis=0, keepdims=True))
            total = total * jnp.exp(top - higher) + jnp.sum(jnp.exp(values - higher), axis=0, keepdims=True)
            ids = lax.broadcasted_iota(jnp.int32, values.shape, 0) + first
            target = target + jnp.sum(jnp.where(ids == wanted, values, 0.0), axis=0, keepdims=True)
            return higher, total, target

        start = (
            jnp.full((1, count), -jnp.inf, jnp.float32),
            jnp.zeros((1, count), jnp.float32),
            jnp.zeros((1, count), jnp.float32),
        )
        top, total, target = lax.fori_loop(0, vocab_rows // STRIPE, stripe, start)
        stats[v] = jnp.concatenate([top, total, target, jnp.zeros((5, count), jnp.float32)], axis=0)

    def stat(offset):
        return remote(
            stats.at[v], stats.at[v], stat_send.at[offset], stat_recv.at[offset], (d, (v + offset) % ranks)
        )

    def stat_arrival(offset):
        source = (v + ranks - offset) % ranks
        remote(
            stats.at[source], stats.at[source], stat_send.at[offset], stat_recv.at[offset], (d, source)
        ).wait_recv()

    for step in range(groups):
        first_level(step)
        if step > 0:
            later_levels(step - 1)
        if step + 1 < groups:
            line_step(step + 1)
        if step == groups - 2:
            matmul()
    for offset in range(1, ranks):
        stat(offset).start()
    later_levels(groups - 1)
    for offset in range(1, ranks):
        stat_arrival(offset)
    top = stats[0, 0:1, :]
    for rank in range(1, ranks):
        top = jnp.maximum(top, stats[rank, 0:1, :])
    total = jnp.zeros_like(top)
    target = jnp.zeros_like(top)
    for rank in range(ranks):
        total += stats[rank, 1:2, :] * jnp.exp(stats[rank, 0:1, :] - top)
        target += stats[rank, 2:3, :]
    logprob[...] = target - top - jnp.log(total)

    for offset in range(1, ranks):
        stat(offset).wait_send()
    for offset in range(replicas):
        for owner in range(owners):
            spread_sent(offset, owner)
    for source in range(ranks):
        for index in range(len(links)):
            cube(source, index).wait_send()
    for group in range(groups):
        pl.when((group <= g) & (g < groups - 1))(lambda: line(group, 1).wait_send())
        pl.when((group >= g) & (g > 0))(lambda: line(group, -1).wait_send())
        pair(group).wait_send()


def assemble(pieces, whole, sem):
    cols = pieces.shape[2]
    copies = [
        pltpu.make_async_copy(pieces.at[source], whole.at[:, pl.ds(source * cols, cols)], sem.at[source])
        for source in range(pieces.shape[0])
    ]
    for copy in copies:
        copy.start()
    for copy in copies:
        copy.wait()


def on_device(hidden, tokens, old_weight, new_weight):
    ranks = lax.axis_size("vocab")
    replicas = lax.axis_size("dp")
    rank = lax.axis_index("vocab")
    own_rows, width = hidden.shape
    vocab_rows = old_weight.shape[0]
    cols = new_weight.shape[1]
    count = own_rows * ranks
    dtype = new_weight.dtype
    groups = ranks // 2
    owners = ranks // replicas
    bits = replicas.bit_length() - 1
    copies = sum(1 if mask == 0 else int(bit > mask.bit_length() - 1) + int(bit < (mask & -mask).bit_length() - 1)
                 for mask in range(replicas) for bit in range(bits) if not mask >> bit & 1)
    dma = pltpu.SemaphoreType.DMA
    anywhere = pl.BlockSpec(memory_space=pl.ANY)
    local = pl.BlockSpec(memory_space=pltpu.VMEM)
    pieces, logprob = pl.pallas_call(
        functools.partial(exchange, replicas, ranks),
        out_shape=(
            pltpu.VMEM((ranks, vocab_rows, cols), dtype),
            jax.ShapeDtypeStruct((1, count), jnp.float32),
        ),
        in_specs=[local, anywhere, anywhere, anywhere],
        out_specs=(local, local),
        scratch_shapes=[
            pltpu.VMEM((count, width), hidden.dtype),
            pltpu.VMEM((vocab_rows, width), old_weight.dtype),
            pltpu.VMEM((STRIPE, count), jnp.float32),
            pltpu.VMEM((ranks, 8, count), jnp.float32),
            dma((1,)), dma((1,)),
            dma((2, groups)), dma((2, groups)), dma((groups,)), dma((groups,)),
            dma((replicas * owners,)), dma((ranks,)),
            dma((ranks, copies)), dma((ranks, copies)),
            dma((ranks,)), dma((ranks,)),
        ],
        compiler_params=pltpu.CompilerParams(has_side_effects=True, vmem_limit_bytes=44 * 1024 * 1024),
        name="exchange",
    )(tokens.reshape(1, count), hidden, old_weight, new_weight)
    logprob = lax.dynamic_slice(logprob[0], (rank * own_rows,), (own_rows,))
    if cols % 128 == 0:
        engine_weight = pl.pallas_call(
            assemble,
            out_shape=jax.ShapeDtypeStruct((vocab_rows, ranks * cols), dtype),
            in_specs=[anywhere],
            out_specs=anywhere,
            scratch_shapes=[dma((ranks,))],
            compiler_params=pltpu.CompilerParams(vmem_limit_bytes=1024 * 1024),
            name="assemble",
        )(pieces)
    else:
        engine_weight = jnp.swapaxes(pieces, 0, 1).reshape(vocab_rows, ranks * cols)
    return (logprob, engine_weight)


def solution(mesh):
    return jax.shard_map(
        on_device,
        mesh=mesh,
        in_specs=(P(("dp", "vocab"), None), P("dp"), P("vocab", None), P("dp", "vocab")),
        out_specs=(P(("dp", "vocab")), P("vocab", None)),
        check_vma=False,
    )
```

```python
import functools

import jax
import jax.numpy as jnp
from jax import lax
from jax.experimental import pallas as pl
from jax.experimental.pallas import tpu as pltpu
from jax.sharding import PartitionSpec as P

MESH = pl.DeviceIdType.MESH
STRIPE = 384


def pick(index, choices):
    value = jnp.int32(choices[0])
    for k in range(1, len(choices)):
        value = jnp.where(index == k, choices[k], value)
    return value


def nearest_first(count):
    return [sorted(range(count), key=lambda other: (abs(other - own), other)) for own in range(count)]


def exchange(
    replicas, ranks, tokens, hidden, old, new, pieces, logprob,
    gathered, weight, logits, stats, relay, local_sem, weight_sem,
    line_send, line_recv, pair_send, pair_recv, relay_send, relay_recv,
    spread_send, spread_recv, cube_send, cube_recv, stat_send, stat_recv,
):
    d = lax.axis_index("dp")
    v = lax.axis_index("vocab")
    owners = ranks // replicas
    groups = ranks // 2
    g, core = v // 2, v % 2
    own_rows = hidden.shape[0]
    vocab_rows = old.shape[0]
    part = vocab_rows // replicas
    half = (part // 2) // 16 * 16
    bits = replicas.bit_length() - 1

    def remote(src, dst, send, recv, device):
        return pltpu.make_async_remote_copy(
            src_ref=src, dst_ref=dst, send_sem=send, recv_sem=recv, device_id=device, device_id_type=MESH
        )

    def rows_of(rank):
        return gathered.at[pl.ds(pl.multiple_of(rank * own_rows, own_rows), own_rows), :]

    def line(group, step, source=None):
        slot = rows_of(2 * group + core)
        way = 0 if step > 0 else 1
        return remote(
            slot if source is None else source, slot, line_send.at[way, group], line_recv.at[way, group],
            (d, v + 2 * step),
        )

    def pair(group, source=None):
        slot = rows_of(2 * group + core)
        return remote(
            slot if source is None else source, slot, pair_send.at[group], pair_recv.at[group], (d, v + 1 - 2 * core)
        )

    def pair_arrival(group):
        slot = rows_of(2 * group + 1 - core)
        return remote(slot, slot, pair_send.at[group], pair_recv.at[group], (d, v + 1 - 2 * core))

    own_copy = pltpu.make_async_copy(hidden, rows_of(v), local_sem.at[0])
    own_copy.start()
    pl.when(g < groups - 1)(lambda: line(g, 1, hidden).start())
    pl.when(g > 0)(lambda: line(g, -1, hidden).start())
    pair(g, hidden).start()

    def line_step(step):
        def below():
            line(g - step, 1).wait_recv()
            pl.when(g < groups - 1)(lambda: line(g - step, 1).start())
            pair(g - step).start()

        def above():
            line(g + step, -1).wait_recv()
            pl.when(g > 0)(lambda: line(g + step, -1).start())
            pair(g + step).start()

        pl.when(g >= step)(below)
        pl.when(g + step < groups)(above)

    def hand(offset, owner):
        target = d ^ offset
        source = new.at[pl.ds(pl.multiple_of(owner * vocab_rows + target * part, 16), part), :]
        slot = relay.at[offset - 1, owner]
        index = (offset - 1) * owners + owner
        return remote(source, slot, relay_send.at[index], relay_recv.at[index], (target, v))

    def spread(offset, owner, stay=False):
        rank = (d ^ offset) * owners + owner
        if offset:
            source = relay.at[offset - 1, owner]
        else:
            source = new.at[pl.ds(pl.multiple_of(owner * vocab_rows + d * part, 16), part), :]
        slot = pieces.at[v, pl.ds(pl.multiple_of(d * part, 16), part), :]
        if stay:
            return pltpu.make_async_copy(source, slot, spread_recv.at[v])
        return remote(source, slot, spread_send.at[offset * owners + owner], spread_recv.at[v], (d, rank))

    def spread_start(offset, owner):
        rank = (d ^ offset) * owners + owner
        pl.when(rank == v)(lambda: spread(offset, owner, stay=True).start())
        pl.when(rank != v)(lambda: spread(offset, owner).start())

    def spread_sent(offset, owner):
        rank = (d ^ offset) * owners + owner
        pl.when(rank != v)(lambda: spread(offset, owner).wait_send())

    def spread_arrival(source):
        slot = pieces.at[source, pl.ds(pl.multiple_of(d * part, 16), part), :]
        pltpu.make_async_copy(slot, slot, spread_recv.at[source]).wait()

    def span(holder, which):
        first, length = {"all": (0, part), "low": (0, half), "high": (half, part - half)}[which]
        return pl.ds(pl.multiple_of(holder * part + first, 16), length)

    links = []
    for mask in range(replicas):
        for bit in range(bits):
            if mask >> bit & 1:
                continue
            if mask == 0:
                links.append((mask, bit, "all"))
                continue
            if bit > mask.bit_length() - 1:
                links.append((mask, bit, "low"))
            if bit < (mask & -mask).bit_length() - 1:
                links.append((mask, bit, "high"))

    def cube(source, index):
        mask, bit, which = links[index]
        slot = pieces.at[source, span(d ^ mask, which), :]
        return remote(slot, slot, cube_send.at[source, index], cube_recv.at[source, index], (d ^ (1 << bit), v))

    def cube_arrival(source, index):
        mask, bit, which = links[index]
        slot = pieces.at[source, span(d ^ mask ^ (1 << bit), which), :]
        remote(slot, slot, cube_send.at[source, index], cube_recv.at[source, index], (d ^ (1 << bit), v)).wait_recv()

    def cube_level(source, level):
        for index, (mask, bit, which) in enumerate(links):
            if mask.bit_count() == level - 1:
                cube_arrival(source, index)
                for onward, (held, _, wanted) in enumerate(links):
                    if held == mask | 1 << bit and which in ("all", wanted):
                        cube(source, onward).start()

    for offset in range(1, replicas):
        for owner in range(owners):
            hand(offset, owner).start()
    for owner in range(owners):
        spread_start(0, owner)

    weight_copy = pltpu.make_async_copy(old, weight, weight_sem.at[0])
    weight_copy.start()

    table = nearest_first(groups)

    def sources(step):
        group = pick(g, [table[own][step] for own in range(groups)])
        return [2 * group, 2 * group + 1]

    def first_level(step):
        for source in sources(step):
            spread_arrival(source)
            for index, (mask, _, _) in enumerate(links):
                if mask == 0:
                    cube(source, index).start()

    def later_levels(step):
        for level in range(1, bits + 1):
            for source in sources(step):
                cube_level(source, level)

    def matmul():
        for group in range(groups):
            pair_arrival(group).wait_recv()
        own_copy.wait()
        weight_copy.wait()
        wanted = tokens[...] - v * vocab_rows
        count = gathered.shape[0]

        def stripe(index, carry):
            top, total, target = carry
            first = pl.multiple_of(index * STRIPE, STRIPE)
            logits[...] = lax.dot_general(
                weight[pl.ds(first, STRIPE), :], gathered[...], (((1,), (1,)), ((), ())),
                preferred_element_type=jnp.float32,
            )
            values = logits[...]
            higher = jnp.maximum(top, jnp.max(values, axis=0, keepdims=True))
            total = total * jnp.exp(top - higher) + jnp.sum(jnp.exp(values - higher), axis=0, keepdims=True)
            ids = lax.broadcasted_iota(jnp.int32, values.shape, 0) + first
            target = target + jnp.sum(jnp.where(ids == wanted, values, 0.0), axis=0, keepdims=True)
            return higher, total, target

        start = (
            jnp.full((1, count), -jnp.inf, jnp.float32),
            jnp.zeros((1, count), jnp.float32),
            jnp.zeros((1, count), jnp.float32),
        )
        top, total, target = lax.fori_loop(0, vocab_rows // STRIPE, stripe, start)
        stats[v] = jnp.concatenate([top, total, target, jnp.zeros((5, count), jnp.float32)], axis=0)

    def stat(offset):
        return remote(
            stats.at[v], stats.at[v], stat_send.at[offset], stat_recv.at[offset], (d, (v + offset) % ranks)
        )

    def stat_arrival(offset):
        source = (v + ranks - offset) % ranks
        remote(
            stats.at[source], stats.at[source], stat_send.at[offset], stat_recv.at[offset], (d, source)
        ).wait_recv()

    for offset in range(1, replicas):
        for owner in range(owners):
            hand(offset, owner).wait_recv()
            spread_start(offset, owner)
    for step in range(groups):
        first_level(step)
        if step > 0:
            later_levels(step - 1)
        if step + 1 < groups:
            line_step(step + 1)
        if step == groups - 2:
            matmul()
    for offset in range(1, ranks):
        stat(offset).start()
    later_levels(groups - 1)
    for offset in range(1, ranks):
        stat_arrival(offset)
    top = stats[0, 0:1, :]
    for rank in range(1, ranks):
        top = jnp.maximum(top, stats[rank, 0:1, :])
    total = jnp.zeros_like(top)
    target = jnp.zeros_like(top)
    for rank in range(ranks):
        total += stats[rank, 1:2, :] * jnp.exp(stats[rank, 0:1, :] - top)
        target += stats[rank, 2:3, :]
    logprob[...] = target - top - jnp.log(total)

    for offset in range(1, ranks):
        stat(offset).wait_send()
    for offset in range(replicas):
        for owner in range(owners):
            spread_sent(offset, owner)
            if offset:
                hand(offset, owner).wait_send()
    for source in range(ranks):
        for index in range(len(links)):
            cube(source, index).wait_send()
    for group in range(groups):
        pl.when((group <= g) & (g < groups - 1))(lambda: line(group, 1).wait_send())
        pl.when((group >= g) & (g > 0))(lambda: line(group, -1).wait_send())
        pair(group).wait_send()


def assemble(pieces, whole, sem):
    cols = pieces.shape[2]
    copies = [
        pltpu.make_async_copy(pieces.at[source], whole.at[:, pl.ds(source * cols, cols)], sem.at[source])
        for source in range(pieces.shape[0])
    ]
    for copy in copies:
        copy.start()
    for copy in copies:
        copy.wait()


def on_device(hidden, tokens, old_weight, new_weight):
    ranks = lax.axis_size("vocab")
    replicas = lax.axis_size("dp")
    rank = lax.axis_index("vocab")
    own_rows, width = hidden.shape
    vocab_rows = old_weight.shape[0]
    cols = new_weight.shape[1]
    count = own_rows * ranks
    dtype = new_weight.dtype
    groups = ranks // 2
    owners = ranks // replicas
    bits = replicas.bit_length() - 1
    copies = sum(1 if mask == 0 else int(bit > mask.bit_length() - 1) + int(bit < (mask & -mask).bit_length() - 1)
                 for mask in range(replicas) for bit in range(bits) if not mask >> bit & 1)
    dma = pltpu.SemaphoreType.DMA
    anywhere = pl.BlockSpec(memory_space=pl.ANY)
    local = pl.BlockSpec(memory_space=pltpu.VMEM)
    pieces, logprob = pl.pallas_call(
        functools.partial(exchange, replicas, ranks),
        out_shape=(
            pltpu.VMEM((ranks, vocab_rows, cols), dtype),
            jax.ShapeDtypeStruct((1, count), jnp.float32),
        ),
        in_specs=[local, anywhere, anywhere, anywhere],
        out_specs=(local, local),
        scratch_shapes=[
            pltpu.VMEM((count, width), hidden.dtype),
            pltpu.VMEM((vocab_rows, width), old_weight.dtype),
            pltpu.VMEM((STRIPE, count), jnp.float32),
            pltpu.VMEM((ranks, 8, count), jnp.float32),
            pltpu.VMEM((replicas - 1, owners, vocab_rows // replicas, cols), dtype),
            dma((1,)), dma((1,)),
            dma((2, groups)), dma((2, groups)), dma((groups,)), dma((groups,)),
            dma(((replicas - 1) * owners,)), dma(((replicas - 1) * owners,)),
            dma((replicas * owners,)), dma((ranks,)),
            dma((ranks, copies)), dma((ranks, copies)),
            dma((ranks,)), dma((ranks,)),
        ],
        compiler_params=pltpu.CompilerParams(has_side_effects=True, vmem_limit_bytes=44 * 1024 * 1024),
        name="exchange",
    )(tokens.reshape(1, count), hidden, old_weight, new_weight)
    logprob = lax.dynamic_slice(logprob[0], (rank * own_rows,), (own_rows,))
    if cols % 128 == 0:
        engine_weight = pl.pallas_call(
            assemble,
            out_shape=jax.ShapeDtypeStruct((vocab_rows, ranks * cols), dtype),
            in_specs=[anywhere],
            out_specs=anywhere,
            scratch_shapes=[dma((ranks,))],
            compiler_params=pltpu.CompilerParams(vmem_limit_bytes=1024 * 1024),
            name="assemble",
        )(pieces)
    else:
        engine_weight = jnp.swapaxes(pieces, 0, 1).reshape(vocab_rows, ranks * cols)
    return (logprob, engine_weight)


def solution(mesh):
    return jax.shard_map(
        on_device,
        mesh=mesh,
        in_specs=(P(("dp", "vocab"), None), P("dp"), P("vocab", None), P("dp", "vocab")),
        out_specs=(P(("dp", "vocab")), P("vocab", None)),
        check_vma=False,
    )
```

```python
import functools

import jax
import jax.numpy as jnp
from jax import lax
from jax.experimental import pallas as pl
from jax.experimental.pallas import tpu as pltpu
from jax.sharding import PartitionSpec as P

MESH = pl.DeviceIdType.MESH
STRIPE = 384


def plan_of(replicas, groups, stripes):
    tasks = [("hand", offset) for offset in range(1, replicas)] + [("line", 0)]
    tasks += [("spread", turn) for turn in range(groups)] + [("first", 0)]
    for turn in range(1, groups):
        tasks += [("first", turn), ("later", turn - 1), ("line", turn)]
    tasks += [("logits", stripe) for stripe in range(stripes)]
    return tasks + [("stats", 0), ("later", groups - 1)]


def exchange(
    replicas, ranks, tokens, hidden, old, new, pieces, logprob,
    gathered, weight, logits, stats, relay, local_sem, weight_sem,
    line_send, line_recv, pair_send, pair_recv, relay_send, relay_recv,
    spread_send, spread_recv, cube_send, cube_recv, stat_send, stat_recv,
):
    d = lax.axis_index("dp")
    v = lax.axis_index("vocab")
    owners = ranks // replicas
    groups = ranks // 2
    g, core = v // 2, v % 2
    own_rows = hidden.shape[0]
    vocab_rows = old.shape[0]
    part = vocab_rows // replicas
    half = (part // 2) // 16 * 16
    bits = replicas.bit_length() - 1

    def remote(src, dst, send, recv, device):
        return pltpu.make_async_remote_copy(
            src_ref=src, dst_ref=dst, send_sem=send, recv_sem=recv, device_id=device, device_id_type=MESH
        )

    def rows_of(rank):
        return gathered.at[pl.ds(pl.multiple_of(rank * own_rows, own_rows), own_rows), :]

    def line(group, step, source=None):
        slot = rows_of(2 * group + core)
        way = 0 if step > 0 else 1
        return remote(
            slot if source is None else source, slot, line_send.at[way, group], line_recv.at[way, group],
            (d, v + 2 * step),
        )

    def pair(group, source=None):
        slot = rows_of(2 * group + core)
        return remote(
            slot if source is None else source, slot, pair_send.at[group], pair_recv.at[group], (d, v + 1 - 2 * core)
        )

    def pair_arrival(group):
        slot = rows_of(2 * group + 1 - core)
        return remote(slot, slot, pair_send.at[group], pair_recv.at[group], (d, v + 1 - 2 * core))

    own_copy = pltpu.make_async_copy(hidden, rows_of(v), local_sem.at[0])
    weight_copy = pltpu.make_async_copy(old, weight, weight_sem.at[0])

    def line_start():
        pl.when(g < groups - 1)(lambda: line(g, 1, hidden).start())
        pl.when(g > 0)(lambda: line(g, -1, hidden).start())
        pair(g, hidden).start()
        own_copy.start()
        weight_copy.start()

    def line_step(step):
        if step == 0:
            return line_start()

        def below():
            line(g - step, 1).wait_recv()
            pl.when(g < groups - 1)(lambda: line(g - step, 1).start())
            pair(g - step).start()

        def above():
            line(g + step, -1).wait_recv()
            pl.when(g > 0)(lambda: line(g + step, -1).start())
            pair(g + step).start()

        pl.when(g >= step)(below)
        pl.when(g + step < groups)(above)

    def hand(offset, owner):
        target = d ^ offset
        source = new.at[pl.ds(pl.multiple_of(owner * vocab_rows + target * part, 16), part), :]
        slot = relay.at[offset - 1, owner]
        index = (offset - 1) * owners + owner
        return remote(source, slot, relay_send.at[index], relay_recv.at[index], (target, v))

    def spread(turn, owner, source, stay=False):
        slot = pieces.at[v, pl.ds(pl.multiple_of(d * part, 16), part), :]
        if stay:
            return pltpu.make_async_copy(source, slot, spread_recv.at[v])
        rank = (g ^ turn) * owners + owner
        return remote(source, slot, spread_send.at[turn * owners + owner], spread_recv.at[v], (d, rank))

    def spread_from(turn, owner, source):
        if turn:
            return spread(turn, owner, source).start()
        pl.when(owner == core)(lambda: spread(turn, owner, source, stay=True).start())
        pl.when(owner != core)(lambda: spread(turn, owner, source).start())

    def spread_turn(turn):
        offset = d ^ g ^ turn

        def own():
            for owner in range(owners):
                first = pl.multiple_of(owner * vocab_rows + d * part, 16)
                spread_from(turn, owner, new.at[pl.ds(first, part), :])

        def handed():
            for owner in range(owners):
                hand(offset, owner).wait_recv()
                spread_from(turn, owner, relay.at[offset - 1, owner])

        pl.when(offset == 0)(own)
        pl.when(offset != 0)(handed)

    def spread_sent(turn, owner):
        def sent():
            spread(turn, owner, relay.at[0, owner]).wait_send()

        if turn:
            sent()
        else:
            pl.when(owner != core)(sent)

    def spread_arrival(source):
        slot = pieces.at[source, pl.ds(pl.multiple_of(d * part, 16), part), :]
        pltpu.make_async_copy(slot, slot, spread_recv.at[source]).wait()

    def span(holder, which):
        first, length = {"all": (0, part), "low": (0, half), "high": (half, part - half)}[which]
        return pl.ds(pl.multiple_of(holder * part + first, 16), length)

    links = []
    for mask in range(replicas):
        for bit in range(bits):
            if mask >> bit & 1:
                continue
            if mask == 0:
                links.append((mask, bit, "all"))
                continue
            if bit > mask.bit_length() - 1:
                links.append((mask, bit, "low"))
            if bit < (mask & -mask).bit_length() - 1:
                links.append((mask, bit, "high"))

    def cube(source, index):
        mask, bit, which = links[index]
        slot = pieces.at[source, span(d ^ mask, which), :]
        return remote(slot, slot, cube_send.at[source, index], cube_recv.at[source, index], (d ^ (1 << bit), v))

    def cube_arrival(source, index):
        mask, bit, which = links[index]
        slot = pieces.at[source, span(d ^ mask ^ (1 << bit), which), :]
        remote(slot, slot, cube_send.at[source, index], cube_recv.at[source, index], (d ^ (1 << bit), v)).wait_recv()

    def cube_level(source, level):
        for index, (mask, bit, which) in enumerate(links):
            if mask.bit_count() == level - 1:
                cube_arrival(source, index)
                for onward, (held, _, wanted) in enumerate(links):
                    if held == mask | 1 << bit and which in ("all", wanted):
                        cube(source, onward).start()

    def sources(turn):
        return [2 * (g ^ turn), 2 * (g ^ turn) + 1]

    def first_level(step):
        for source in sources(step):
            spread_arrival(source)
            for index, (mask, _, _) in enumerate(links):
                if mask == 0:
                    cube(source, index).start()

    def later_levels(step):
        for level in range(1, bits):
            for source in sources(step):
                cube_level(source, level)

    def logits_stripe(index):
        count = gathered.shape[0]
        if index == 0:
            for group in range(groups):
                pair_arrival(group).wait_recv()
            own_copy.wait()
            weight_copy.wait()
            floor = jnp.full((1, count), -jnp.inf, jnp.float32)
            stats[v] = jnp.concatenate([floor, jnp.zeros((7, count), jnp.float32)], axis=0)
        first = index * STRIPE
        logits[...] = lax.dot_general(
            weight[pl.ds(first, STRIPE), :], gathered[...], (((1,), (1,)), ((), ())),
            preferred_element_type=jnp.float32,
        )
        values = logits[...]
        top = stats[v, 0:1, :]
        higher = jnp.maximum(top, jnp.max(values, axis=0, keepdims=True))
        total = stats[v, 1:2, :] * jnp.exp(top - higher)
        total += jnp.sum(jnp.exp(values - higher), axis=0, keepdims=True)
        ids = lax.broadcasted_iota(jnp.int32, values.shape, 0) + (first + v * vocab_rows)
        target = jnp.sum(jnp.where(ids == tokens[...], values, 0.0), axis=0, keepdims=True)
        stats[v, 0:1, :] = higher
        stats[v, 1:2, :] = total
        stats[v, 2:3, :] += target

    def stat(offset):
        return remote(
            stats.at[v], stats.at[v], stat_send.at[offset], stat_recv.at[offset], (d, (v + offset) % ranks)
        )

    def stat_arrival(offset):
        source = (v + ranks - offset) % ranks
        remote(
            stats.at[source], stats.at[source], stat_send.at[offset], stat_recv.at[offset], (d, source)
        ).wait_recv()

    def hand_start(offset):
        for owner in range(owners):
            hand(offset, owner).start()

    def stats_start(_):
        for offset in range(1, ranks):
            stat(offset).start()

    run = {
        "hand": hand_start, "line": line_step, "spread": spread_turn, "first": first_level,
        "later": later_levels, "logits": logits_stripe, "stats": stats_start,
    }
    for task, index in plan_of(replicas, groups, vocab_rows // STRIPE):
        run[task](index)
    for source in range(ranks):
        cube_level(source, bits)
    for offset in range(1, ranks):
        stat_arrival(offset)
    top = stats[0, 0:1, :]
    for rank in range(1, ranks):
        top = jnp.maximum(top, stats[rank, 0:1, :])
    total = jnp.zeros_like(top)
    target = jnp.zeros_like(top)
    for rank in range(ranks):
        total += stats[rank, 1:2, :] * jnp.exp(stats[rank, 0:1, :] - top)
        target += stats[rank, 2:3, :]
    logprob[...] = target - top - jnp.log(total)

    for offset in range(1, ranks):
        stat(offset).wait_send()
    for owner in range(owners):
        for turn in range(groups):
            spread_sent(turn, owner)
        for offset in range(1, replicas):
            hand(offset, owner).wait_send()
    for source in range(ranks):
        for index in range(len(links)):
            cube(source, index).wait_send()
    for group in range(groups):
        pl.when((group <= g) & (g < groups - 1))(lambda: line(group, 1).wait_send())
        pl.when((group >= g) & (g > 0))(lambda: line(group, -1).wait_send())
        pair(group).wait_send()


def assemble(pieces, whole, sem):
    cols = pieces.shape[2]
    copies = [
        pltpu.make_async_copy(pieces.at[source], whole.at[:, pl.ds(source * cols, cols)], sem.at[source])
        for source in range(pieces.shape[0])
    ]
    for copy in copies:
        copy.start()
    for copy in copies:
        copy.wait()


def on_device(hidden, tokens, old_weight, new_weight):
    ranks = lax.axis_size("vocab")
    replicas = lax.axis_size("dp")
    rank = lax.axis_index("vocab")
    own_rows, width = hidden.shape
    vocab_rows = old_weight.shape[0]
    cols = new_weight.shape[1]
    count = own_rows * ranks
    dtype = new_weight.dtype
    groups = ranks // 2
    owners = ranks // replicas
    assert groups == replicas == 1 << (replicas.bit_length() - 1)
    bits = replicas.bit_length() - 1
    copies = sum(1 if mask == 0 else int(bit > mask.bit_length() - 1) + int(bit < (mask & -mask).bit_length() - 1)
                 for mask in range(replicas) for bit in range(bits) if not mask >> bit & 1)
    dma = pltpu.SemaphoreType.DMA
    anywhere = pl.BlockSpec(memory_space=pl.ANY)
    local = pl.BlockSpec(memory_space=pltpu.VMEM)
    pieces, logprob = pl.pallas_call(
        functools.partial(exchange, replicas, ranks),
        out_shape=(
            pltpu.VMEM((ranks, vocab_rows, cols), dtype),
            jax.ShapeDtypeStruct((1, count), jnp.float32),
        ),
        in_specs=[local, anywhere, anywhere, anywhere],
        out_specs=(local, local),
        scratch_shapes=[
            pltpu.VMEM((count, width), hidden.dtype),
            pltpu.VMEM((vocab_rows, width), old_weight.dtype),
            pltpu.VMEM((STRIPE, count), jnp.float32),
            pltpu.VMEM((ranks, 8, count), jnp.float32),
            pltpu.VMEM((replicas - 1, owners, vocab_rows // replicas, cols), dtype),
            dma((1,)), dma((1,)),
            dma((2, groups)), dma((2, groups)), dma((groups,)), dma((groups,)),
            dma(((replicas - 1) * owners,)), dma(((replicas - 1) * owners,)),
            dma((groups * owners,)), dma((ranks,)),
            dma((ranks, copies)), dma((ranks, copies)),
            dma((ranks,)), dma((ranks,)),
        ],
        compiler_params=pltpu.CompilerParams(has_side_effects=True, vmem_limit_bytes=44 * 1024 * 1024),
        name="exchange",
    )(tokens.reshape(1, count), hidden, old_weight, new_weight)
    logprob = lax.dynamic_slice(logprob[0], (rank * own_rows,), (own_rows,))
    if cols % 128 == 0:
        engine_weight = pl.pallas_call(
            assemble,
            out_shape=jax.ShapeDtypeStruct((vocab_rows, ranks * cols), dtype),
            in_specs=[anywhere],
            out_specs=anywhere,
            scratch_shapes=[dma((ranks,))],
            compiler_params=pltpu.CompilerParams(vmem_limit_bytes=1024 * 1024),
            name="assemble",
        )(pieces)
    else:
        engine_weight = jnp.swapaxes(pieces, 0, 1).reshape(vocab_rows, ranks * cols)
    return (logprob, engine_weight)


def solution(mesh):
    return jax.shard_map(
        on_device,
        mesh=mesh,
        in_specs=(P(("dp", "vocab"), None), P("dp"), P("vocab", None), P("dp", "vocab")),
        out_specs=(P(("dp", "vocab")), P("vocab", None)),
        check_vma=False,
    )
```

```python
import functools

import jax
import jax.numpy as jnp
from jax import lax
from jax.experimental import pallas as pl
from jax.experimental.pallas import tpu as pltpu
from jax.sharding import PartitionSpec as P

MESH = pl.DeviceIdType.MESH
STRIPE = 384


def plan_of(replicas, groups, stripes):
    tasks = [("hand", 2), ("line", 0), ("hand", 1)] + [("hand", offset) for offset in range(3, replicas)]
    tasks += [("line", 1), ("spread", 1), ("spread", 2), ("spread", 0)]
    tasks += [("spread", turn) for turn in range(3, groups)]
    tasks += [("first", 0), ("later", 0), ("first", 1), ("first", 2), ("line", 2), ("later", 1), ("later", 2)]
    for turn in range(3, groups):
        tasks += [("later", turn - 1)] * (turn > 3) + [("line", turn), ("first", turn)]
    tasks += [("logits", stripe) for stripe in range(stripes)]
    return tasks + [("stats", 0), ("later", groups - 1)]


def exchange(
    replicas, ranks, tokens, hidden, old, new, pieces, logprob,
    gathered, weight, logits, stats, relay, local_sem, weight_sem,
    line_send, line_recv, pair_send, pair_recv, relay_send, relay_recv,
    spread_send, spread_recv, cube_send, cube_recv, stat_send, stat_recv,
):
    d = lax.axis_index("dp")
    v = lax.axis_index("vocab")
    owners = ranks // replicas
    groups = ranks // 2
    g, core = v // 2, v % 2
    own_rows = hidden.shape[0]
    vocab_rows = old.shape[0]
    part = vocab_rows // replicas
    half = (part // 2) // 16 * 16
    bits = replicas.bit_length() - 1

    def remote(src, dst, send, recv, device):
        return pltpu.make_async_remote_copy(
            src_ref=src, dst_ref=dst, send_sem=send, recv_sem=recv, device_id=device, device_id_type=MESH
        )

    def rows_of(rank):
        return gathered.at[pl.ds(pl.multiple_of(rank * own_rows, own_rows), own_rows), :]

    def line(group, step, source=None):
        slot = rows_of(2 * group + core)
        way = 0 if step > 0 else 1
        return remote(
            slot if source is None else source, slot, line_send.at[way, group], line_recv.at[way, group],
            (d, v + 2 * step),
        )

    def pair(group, source=None):
        slot = rows_of(2 * group + core)
        return remote(
            slot if source is None else source, slot, pair_send.at[group], pair_recv.at[group], (d, v + 1 - 2 * core)
        )

    def pair_arrival(group):
        slot = rows_of(2 * group + 1 - core)
        return remote(slot, slot, pair_send.at[group], pair_recv.at[group], (d, v + 1 - 2 * core))

    own_copy = pltpu.make_async_copy(hidden, rows_of(v), local_sem.at[0])
    weight_copy = pltpu.make_async_copy(old, weight, weight_sem.at[0])

    def line_start():
        pl.when(g < groups - 1)(lambda: line(g, 1, hidden).start())
        pl.when(g > 0)(lambda: line(g, -1, hidden).start())
        pair(g, hidden).start()
        own_copy.start()
        weight_copy.start()

    def line_step(step):
        if step == 0:
            return line_start()

        def below():
            line(g - step, 1).wait_recv()
            pl.when(g < groups - 1)(lambda: line(g - step, 1).start())
            pair(g - step).start()

        def above():
            line(g + step, -1).wait_recv()
            pl.when(g > 0)(lambda: line(g + step, -1).start())
            pair(g + step).start()

        pl.when(g >= step)(below)
        pl.when(g + step < groups)(above)

    def hand(offset, owner):
        target = d ^ offset
        source = new.at[pl.ds(pl.multiple_of(owner * vocab_rows + target * part, 16), part), :]
        slot = relay.at[offset - 1, owner]
        index = (offset - 1) * owners + owner
        return remote(source, slot, relay_send.at[index], relay_recv.at[index], (target, v))

    def spread(turn, owner, source, stay=False):
        slot = pieces.at[v, pl.ds(pl.multiple_of(d * part, 16), part), :]
        if stay:
            return pltpu.make_async_copy(source, slot, spread_recv.at[v])
        rank = (g ^ turn) * owners + owner
        return remote(source, slot, spread_send.at[turn * owners + owner], spread_recv.at[v], (d, rank))

    def spread_from(turn, owner, source):
        if turn:
            return spread(turn, owner, source).start()
        pl.when(owner == core)(lambda: spread(turn, owner, source, stay=True).start())
        pl.when(owner != core)(lambda: spread(turn, owner, source).start())

    def spread_turn(turn):
        offset = d ^ g ^ turn

        def own():
            for owner in range(owners):
                first = pl.multiple_of(owner * vocab_rows + d * part, 16)
                spread_from(turn, owner, new.at[pl.ds(first, part), :])

        def handed():
            for owner in range(owners):
                hand(offset, owner).wait_recv()
                spread_from(turn, owner, relay.at[offset - 1, owner])

        pl.when(offset == 0)(own)
        pl.when(offset != 0)(handed)

    def spread_sent(turn, owner):
        def sent():
            spread(turn, owner, relay.at[0, owner]).wait_send()

        if turn:
            sent()
        else:
            pl.when(owner != core)(sent)

    def spread_arrival(source):
        slot = pieces.at[source, pl.ds(pl.multiple_of(d * part, 16), part), :]
        pltpu.make_async_copy(slot, slot, spread_recv.at[source]).wait()

    def span(holder, which):
        first, length = {"all": (0, part), "low": (0, half), "high": (half, part - half)}[which]
        return pl.ds(pl.multiple_of(holder * part + first, 16), length)

    links = []
    for mask in range(replicas):
        for bit in range(bits):
            if mask >> bit & 1:
                continue
            if mask == 0:
                links.append((mask, bit, "all"))
                continue
            if bit > mask.bit_length() - 1:
                links.append((mask, bit, "low"))
            if bit < (mask & -mask).bit_length() - 1:
                links.append((mask, bit, "high"))

    def cube(source, index):
        mask, bit, which = links[index]
        slot = pieces.at[source, span(d ^ mask, which), :]
        return remote(slot, slot, cube_send.at[source, index], cube_recv.at[source, index], (d ^ (1 << bit), v))

    def cube_arrival(source, index):
        mask, bit, which = links[index]
        slot = pieces.at[source, span(d ^ mask ^ (1 << bit), which), :]
        remote(slot, slot, cube_send.at[source, index], cube_recv.at[source, index], (d ^ (1 << bit), v)).wait_recv()

    def cube_level(source, level):
        for index, (mask, bit, which) in enumerate(links):
            if mask.bit_count() == level - 1:
                cube_arrival(source, index)
                for onward, (held, _, wanted) in enumerate(links):
                    if held == mask | 1 << bit and which in ("all", wanted):
                        cube(source, onward).start()

    def sources(turn):
        return [2 * (g ^ turn), 2 * (g ^ turn) + 1]

    def first_level(step):
        for source in sources(step):
            spread_arrival(source)
            for index, (mask, _, _) in enumerate(links):
                if mask == 0:
                    cube(source, index).start()

    def later_levels(step):
        for level in range(1, bits):
            for source in sources(step):
                cube_level(source, level)

    def logits_stripe(index):
        count = gathered.shape[0]
        if index == 0:
            for group in range(groups):
                pair_arrival(group).wait_recv()
            own_copy.wait()
            weight_copy.wait()
            floor = jnp.full((1, count), -jnp.inf, jnp.float32)
            stats[v] = jnp.concatenate([floor, jnp.zeros((7, count), jnp.float32)], axis=0)
        first = index * STRIPE
        logits[...] = lax.dot_general(
            weight[pl.ds(first, STRIPE), :], gathered[...], (((1,), (1,)), ((), ())),
            preferred_element_type=jnp.float32,
        )
        values = logits[...]
        top = stats[v, 0:1, :]
        higher = jnp.maximum(top, jnp.max(values, axis=0, keepdims=True))
        total = stats[v, 1:2, :] * jnp.exp(top - higher)
        total += jnp.sum(jnp.exp(values - higher), axis=0, keepdims=True)
        ids = lax.broadcasted_iota(jnp.int32, values.shape, 0) + (first + v * vocab_rows)
        target = jnp.sum(jnp.where(ids == tokens[...], values, 0.0), axis=0, keepdims=True)
        stats[v, 0:1, :] = higher
        stats[v, 1:2, :] = total
        stats[v, 2:3, :] += target

    def stat(offset):
        return remote(
            stats.at[v], stats.at[v], stat_send.at[offset], stat_recv.at[offset], (d, (v + offset) % ranks)
        )

    def stat_arrival(offset):
        source = (v + ranks - offset) % ranks
        remote(
            stats.at[source], stats.at[source], stat_send.at[offset], stat_recv.at[offset], (d, source)
        ).wait_recv()

    def hand_start(offset):
        for owner in range(owners):
            hand(offset, owner).start()

    def stats_start(_):
        for offset in range(1, ranks):
            stat(offset).start()

    run = {
        "hand": hand_start, "line": line_step, "spread": spread_turn, "first": first_level,
        "later": later_levels, "logits": logits_stripe, "stats": stats_start,
    }
    for task, index in plan_of(replicas, groups, vocab_rows // STRIPE):
        run[task](index)
    for source in range(ranks):
        cube_level(source, bits)
    for offset in range(1, ranks):
        stat_arrival(offset)
    top = stats[0, 0:1, :]
    for rank in range(1, ranks):
        top = jnp.maximum(top, stats[rank, 0:1, :])
    total = jnp.zeros_like(top)
    target = jnp.zeros_like(top)
    for rank in range(ranks):
        total += stats[rank, 1:2, :] * jnp.exp(stats[rank, 0:1, :] - top)
        target += stats[rank, 2:3, :]
    logprob[...] = target - top - jnp.log(total)

    for offset in range(1, ranks):
        stat(offset).wait_send()
    for owner in range(owners):
        for turn in range(groups):
            spread_sent(turn, owner)
        for offset in range(1, replicas):
            hand(offset, owner).wait_send()
    for source in range(ranks):
        for index in range(len(links)):
            cube(source, index).wait_send()
    for group in range(groups):
        pl.when((group <= g) & (g < groups - 1))(lambda: line(group, 1).wait_send())
        pl.when((group >= g) & (g > 0))(lambda: line(group, -1).wait_send())
        pair(group).wait_send()


def assemble(pieces, whole, sem):
    cols = pieces.shape[2]
    copies = [
        pltpu.make_async_copy(pieces.at[source], whole.at[:, pl.ds(source * cols, cols)], sem.at[source])
        for source in range(pieces.shape[0])
    ]
    for copy in copies:
        copy.start()
    for copy in copies:
        copy.wait()


def on_device(hidden, tokens, old_weight, new_weight):
    ranks = lax.axis_size("vocab")
    replicas = lax.axis_size("dp")
    rank = lax.axis_index("vocab")
    own_rows, width = hidden.shape
    vocab_rows = old_weight.shape[0]
    cols = new_weight.shape[1]
    count = own_rows * ranks
    dtype = new_weight.dtype
    groups = ranks // 2
    owners = ranks // replicas
    assert groups == replicas == 1 << (replicas.bit_length() - 1)
    bits = replicas.bit_length() - 1
    copies = sum(1 if mask == 0 else int(bit > mask.bit_length() - 1) + int(bit < (mask & -mask).bit_length() - 1)
                 for mask in range(replicas) for bit in range(bits) if not mask >> bit & 1)
    dma = pltpu.SemaphoreType.DMA
    anywhere = pl.BlockSpec(memory_space=pl.ANY)
    local = pl.BlockSpec(memory_space=pltpu.VMEM)
    pieces, logprob = pl.pallas_call(
        functools.partial(exchange, replicas, ranks),
        out_shape=(
            pltpu.VMEM((ranks, vocab_rows, cols), dtype),
            jax.ShapeDtypeStruct((1, count), jnp.float32),
        ),
        in_specs=[local, anywhere, anywhere, anywhere],
        out_specs=(local, local),
        scratch_shapes=[
            pltpu.VMEM((count, width), hidden.dtype),
            pltpu.VMEM((vocab_rows, width), old_weight.dtype),
            pltpu.VMEM((STRIPE, count), jnp.float32),
            pltpu.VMEM((ranks, 8, count), jnp.float32),
            pltpu.VMEM((replicas - 1, owners, vocab_rows // replicas, cols), dtype),
            dma((1,)), dma((1,)),
            dma((2, groups)), dma((2, groups)), dma((groups,)), dma((groups,)),
            dma(((replicas - 1) * owners,)), dma(((replicas - 1) * owners,)),
            dma((groups * owners,)), dma((ranks,)),
            dma((ranks, copies)), dma((ranks, copies)),
            dma((ranks,)), dma((ranks,)),
        ],
        compiler_params=pltpu.CompilerParams(has_side_effects=True, vmem_limit_bytes=44 * 1024 * 1024),
        name="exchange",
    )(tokens.reshape(1, count), hidden, old_weight, new_weight)
    logprob = lax.dynamic_slice(logprob[0], (rank * own_rows,), (own_rows,))
    if cols % 128 == 0:
        engine_weight = pl.pallas_call(
            assemble,
            out_shape=jax.ShapeDtypeStruct((vocab_rows, ranks * cols), dtype),
            in_specs=[anywhere],
            out_specs=anywhere,
            scratch_shapes=[dma((ranks,))],
            compiler_params=pltpu.CompilerParams(vmem_limit_bytes=1024 * 1024),
            name="assemble",
        )(pieces)
    else:
        engine_weight = jnp.swapaxes(pieces, 0, 1).reshape(vocab_rows, ranks * cols)
    return (logprob, engine_weight)


def solution(mesh):
    return jax.shard_map(
        on_device,
        mesh=mesh,
        in_specs=(P(("dp", "vocab"), None), P("dp"), P("vocab", None), P("dp", "vocab")),
        out_specs=(P(("dp", "vocab")), P("vocab", None)),
        check_vma=False,
    )
```

```python
import functools

import jax
import jax.numpy as jnp
from jax import lax
from jax.experimental import pallas as pl
from jax.experimental.pallas import tpu as pltpu
from jax.sharding import PartitionSpec as P

MESH = pl.DeviceIdType.MESH
STRIPE = 384


def plan_of(replicas, groups, stripes):
    tasks = [("hand", 2), ("line", 0), ("hand", 1)] + [("hand", offset) for offset in range(3, replicas)]
    tasks += [("line", 1), ("spread", 1), ("spread", 2), ("spread", 0)]
    tasks += [("spread", turn) for turn in range(3, groups)]
    tasks += [("first", 0), ("later", 0), ("first", 1), ("first", 2), ("line", 2), ("later", 1), ("later", 2)]
    for turn in range(3, groups):
        tasks += [("later", turn - 1)] * (turn > 3) + [("line", turn), ("first", turn)]
    tasks += [("logits", stripe) for stripe in range(stripes)]
    return tasks + [("stats", 0), ("later", groups - 1)]


def exchange(
    replicas, ranks, tokens, hidden, old, new, pieces, logprob,
    gathered, weight, logits, stats, relay, local_sem, weight_sem,
    line_send, line_recv, pair_send, pair_recv, relay_send, relay_recv,
    spread_send, spread_recv, cube_send, cube_recv, stat_send, stat_recv,
):
    d = lax.axis_index("dp")
    v = lax.axis_index("vocab")
    owners = ranks // replicas
    groups = ranks // 2
    g, core = v // 2, v % 2
    own_rows = hidden.shape[0]
    vocab_rows = old.shape[0]
    part = vocab_rows // replicas
    half = (part // 2) // 16 * 16
    bits = replicas.bit_length() - 1

    def remote(src, dst, send, recv, device):
        return pltpu.make_async_remote_copy(
            src_ref=src, dst_ref=dst, send_sem=send, recv_sem=recv, device_id=device, device_id_type=MESH
        )

    def rows_of(rank):
        return gathered.at[pl.ds(pl.multiple_of(rank * own_rows, own_rows), own_rows), :]

    def line(group, step, source=None):
        slot = rows_of(2 * group + core)
        way = 0 if step > 0 else 1
        return remote(
            slot if source is None else source, slot, line_send.at[way, group], line_recv.at[way, group],
            (d, v + 2 * step),
        )

    def pair(group, source=None):
        slot = rows_of(2 * group + core)
        return remote(
            slot if source is None else source, slot, pair_send.at[group], pair_recv.at[group], (d, v + 1 - 2 * core)
        )

    def pair_arrival(group):
        slot = rows_of(2 * group + 1 - core)
        return remote(slot, slot, pair_send.at[group], pair_recv.at[group], (d, v + 1 - 2 * core))

    ready = pltpu.get_barrier_semaphore()
    for offset in range(1, replicas):
        pl.semaphore_signal(ready, inc=1, device_id=(d ^ offset, v), device_id_type=MESH)
    for offset in range(1, ranks):
        pl.semaphore_signal(ready, inc=1, device_id=(d, (v + offset) % ranks), device_id_type=MESH)

    own_copy = pltpu.make_async_copy(hidden, rows_of(v), local_sem.at[0])
    weight_copy = pltpu.make_async_copy(old, weight, weight_sem.at[0])

    def line_start():
        pl.when(g < groups - 1)(lambda: line(g, 1, hidden).start())
        pl.when(g > 0)(lambda: line(g, -1, hidden).start())
        pair(g, hidden).start()

    def line_step(step):
        if step == 0:
            return line_start()

        def below():
            line(g - step, 1).wait_recv()
            pl.when(g < groups - 1)(lambda: line(g - step, 1).start())
            pair(g - step).start()

        def above():
            line(g + step, -1).wait_recv()
            pl.when(g > 0)(lambda: line(g + step, -1).start())
            pair(g + step).start()

        pl.when(g >= step)(below)
        pl.when(g + step < groups)(above)

    def hand(offset, owner):
        target = d ^ offset
        source = new.at[pl.ds(pl.multiple_of(owner * vocab_rows + target * part, 16), part), :]
        slot = relay.at[offset - 1, owner]
        index = (offset - 1) * owners + owner
        return remote(source, slot, relay_send.at[index], relay_recv.at[index], (target, v))

    def spread(turn, owner, source, stay=False):
        slot = pieces.at[v, pl.ds(pl.multiple_of(d * part, 16), part), :]
        if stay:
            return pltpu.make_async_copy(source, slot, spread_recv.at[v])
        rank = (g ^ turn) * owners + owner
        return remote(source, slot, spread_send.at[turn * owners + owner], spread_recv.at[v], (d, rank))

    def spread_from(turn, owner, source):
        if turn:
            return spread(turn, owner, source).start()
        pl.when(owner == core)(lambda: spread(turn, owner, source, stay=True).start())
        pl.when(owner != core)(lambda: spread(turn, owner, source).start())

    def spread_turn(turn):
        offset = d ^ g ^ turn

        def own():
            for owner in range(owners):
                first = pl.multiple_of(owner * vocab_rows + d * part, 16)
                spread_from(turn, owner, new.at[pl.ds(first, part), :])

        def handed():
            for owner in range(owners):
                hand(offset, owner).wait_recv()
                spread_from(turn, owner, relay.at[offset - 1, owner])

        pl.when(offset == 0)(own)
        pl.when(offset != 0)(handed)

    def spread_sent(turn, owner):
        def sent():
            spread(turn, owner, relay.at[0, owner]).wait_send()

        if turn:
            sent()
        else:
            pl.when(owner != core)(sent)

    def spread_arrival(source):
        slot = pieces.at[source, pl.ds(pl.multiple_of(d * part, 16), part), :]
        pltpu.make_async_copy(slot, slot, spread_recv.at[source]).wait()

    def span(holder, which):
        first, length = {"all": (0, part), "low": (0, half), "high": (half, part - half)}[which]
        return pl.ds(pl.multiple_of(holder * part + first, 16), length)

    links = []
    for mask in range(replicas):
        for bit in range(bits):
            if mask >> bit & 1:
                continue
            if mask == 0:
                links.append((mask, bit, "all"))
                continue
            if bit > mask.bit_length() - 1:
                links.append((mask, bit, "low"))
            if bit < (mask & -mask).bit_length() - 1:
                links.append((mask, bit, "high"))

    def cube(source, index):
        mask, bit, which = links[index]
        slot = pieces.at[source, span(d ^ mask, which), :]
        return remote(slot, slot, cube_send.at[source, index], cube_recv.at[source, index], (d ^ (1 << bit), v))

    def cube_arrival(source, index):
        mask, bit, which = links[index]
        slot = pieces.at[source, span(d ^ mask ^ (1 << bit), which), :]
        remote(slot, slot, cube_send.at[source, index], cube_recv.at[source, index], (d ^ (1 << bit), v)).wait_recv()

    def cube_level(source, level):
        for index, (mask, bit, which) in enumerate(links):
            if mask.bit_count() == level - 1:
                cube_arrival(source, index)
                for onward, (held, _, wanted) in enumerate(links):
                    if held == mask | 1 << bit and which in ("all", wanted):
                        cube(source, onward).start()

    def sources(turn):
        return [2 * (g ^ turn), 2 * (g ^ turn) + 1]

    def first_level(step):
        for source in sources(step):
            spread_arrival(source)
            for index, (mask, _, _) in enumerate(links):
                if mask == 0:
                    cube(source, index).start()

    def later_levels(step):
        for level in range(1, bits):
            for source in sources(step):
                cube_level(source, level)

    def logits_stripe(index):
        count = gathered.shape[0]
        if index == 0:
            for group in range(groups):
                pair_arrival(group).wait_recv()
            own_copy.wait()
            weight_copy.wait()
            floor = jnp.full((1, count), -jnp.inf, jnp.float32)
            stats[v] = jnp.concatenate([floor, jnp.zeros((7, count), jnp.float32)], axis=0)
        first = index * STRIPE
        logits[...] = lax.dot_general(
            weight[pl.ds(first, STRIPE), :], gathered[...], (((1,), (1,)), ((), ())),
            preferred_element_type=jnp.float32,
        )
        values = logits[...]
        top = stats[v, 0:1, :]
        higher = jnp.maximum(top, jnp.max(values, axis=0, keepdims=True))
        total = stats[v, 1:2, :] * jnp.exp(top - higher)
        total += jnp.sum(jnp.exp(values - higher), axis=0, keepdims=True)
        ids = lax.broadcasted_iota(jnp.int32, values.shape, 0) + (first + v * vocab_rows)
        target = jnp.sum(jnp.where(ids == tokens[...], values, 0.0), axis=0, keepdims=True)
        stats[v, 0:1, :] = higher
        stats[v, 1:2, :] = total
        stats[v, 2:3, :] += target

    def stat(offset):
        return remote(
            stats.at[v], stats.at[v], stat_send.at[offset], stat_recv.at[offset], (d, (v + offset) % ranks)
        )

    def stat_arrival(offset):
        source = (v + ranks - offset) % ranks
        remote(
            stats.at[source], stats.at[source], stat_send.at[offset], stat_recv.at[offset], (d, source)
        ).wait_recv()

    def hand_start(offset):
        for owner in range(owners):
            hand(offset, owner).start()

    def stats_start(_):
        for offset in range(1, ranks):
            stat(offset).start()

    run = {
        "hand": hand_start, "line": line_step, "spread": spread_turn, "first": first_level,
        "later": later_levels, "logits": logits_stripe, "stats": stats_start,
    }
    own_copy.start()
    weight_copy.start()
    pl.semaphore_wait(ready, replicas + ranks - 2)
    for task, index in plan_of(replicas, groups, vocab_rows // STRIPE):
        run[task](index)
    for source in range(ranks):
        cube_level(source, bits)
    for offset in range(1, ranks):
        stat_arrival(offset)
    top = stats[0, 0:1, :]
    for rank in range(1, ranks):
        top = jnp.maximum(top, stats[rank, 0:1, :])
    total = jnp.zeros_like(top)
    target = jnp.zeros_like(top)
    for rank in range(ranks):
        total += stats[rank, 1:2, :] * jnp.exp(stats[rank, 0:1, :] - top)
        target += stats[rank, 2:3, :]
    result = target - top - jnp.log(total)
    for rank in range(ranks):
        own = result[:, rank * own_rows : (rank + 1) * own_rows]
        pl.when(v == rank)(lambda: logprob.__setitem__((slice(0, 1), slice(0, own_rows)), own))

    for offset in range(1, ranks):
        stat(offset).wait_send()
    for owner in range(owners):
        for turn in range(groups):
            spread_sent(turn, owner)
        for offset in range(1, replicas):
            hand(offset, owner).wait_send()
    for source in range(ranks):
        for index in range(len(links)):
            cube(source, index).wait_send()
    for group in range(groups):
        pl.when((group <= g) & (g < groups - 1))(lambda: line(group, 1).wait_send())
        pl.when((group >= g) & (g > 0))(lambda: line(group, -1).wait_send())
        pair(group).wait_send()


def assemble(pieces, result, whole, logprob, sem):
    cols = pieces.shape[2]
    copies = [
        pltpu.make_async_copy(pieces.at[source], whole.at[:, pl.ds(source * cols, cols)], sem.at[source])
        for source in range(pieces.shape[0])
    ]
    for copy in copies:
        copy.start()
    logprob[...] = result[...]
    for copy in copies:
        copy.wait()


def on_device(hidden, tokens, old_weight, new_weight):
    ranks = lax.axis_size("vocab")
    replicas = lax.axis_size("dp")
    own_rows, width = hidden.shape
    vocab_rows = old_weight.shape[0]
    cols = new_weight.shape[1]
    count = own_rows * ranks
    dtype = new_weight.dtype
    groups = ranks // 2
    owners = ranks // replicas
    assert groups == replicas == 1 << (replicas.bit_length() - 1)
    bits = replicas.bit_length() - 1
    copies = sum(1 if mask == 0 else int(bit > mask.bit_length() - 1) + int(bit < (mask & -mask).bit_length() - 1)
                 for mask in range(replicas) for bit in range(bits) if not mask >> bit & 1)
    dma = pltpu.SemaphoreType.DMA
    anywhere = pl.BlockSpec(memory_space=pl.ANY)
    local = pl.BlockSpec(memory_space=pltpu.VMEM)
    pieces, logprob = pl.pallas_call(
        functools.partial(exchange, replicas, ranks),
        out_shape=(
            pltpu.VMEM((ranks, vocab_rows, cols), dtype),
            pltpu.VMEM((1, own_rows), jnp.float32),
        ),
        in_specs=[local, anywhere, anywhere, anywhere],
        out_specs=(local, local),
        scratch_shapes=[
            pltpu.VMEM((count, width), hidden.dtype),
            pltpu.VMEM((vocab_rows, width), old_weight.dtype),
            pltpu.VMEM((STRIPE, count), jnp.float32),
            pltpu.VMEM((ranks, 8, count), jnp.float32),
            pltpu.VMEM((replicas - 1, owners, vocab_rows // replicas, cols), dtype),
            dma((1,)), dma((1,)),
            dma((2, groups)), dma((2, groups)), dma((groups,)), dma((groups,)),
            dma(((replicas - 1) * owners,)), dma(((replicas - 1) * owners,)),
            dma((groups * owners,)), dma((ranks,)),
            dma((ranks, copies)), dma((ranks, copies)),
            dma((ranks,)), dma((ranks,)),
        ],
        compiler_params=pltpu.CompilerParams(
            collective_id=0, has_side_effects=True, vmem_limit_bytes=44 * 1024 * 1024
        ),
        name="exchange",
    )(tokens.reshape(1, count), hidden, old_weight, new_weight)
    if cols % 128 == 0:
        engine_weight, logprob = pl.pallas_call(
            assemble,
            out_shape=(
                jax.ShapeDtypeStruct((vocab_rows, ranks * cols), dtype),
                jax.ShapeDtypeStruct((1, own_rows), jnp.float32),
            ),
            in_specs=[anywhere, local],
            out_specs=(anywhere, local),
            scratch_shapes=[dma((ranks,))],
            compiler_params=pltpu.CompilerParams(vmem_limit_bytes=1024 * 1024),
            name="assemble",
        )(pieces, logprob)
    else:
        engine_weight = jnp.swapaxes(pieces, 0, 1).reshape(vocab_rows, ranks * cols)
    return (logprob.reshape(own_rows), engine_weight)


def solution(mesh):
    return jax.shard_map(
        on_device,
        mesh=mesh,
        in_specs=(P(("dp", "vocab"), None), P("dp"), P("vocab", None), P("dp", "vocab")),
        out_specs=(P(("dp", "vocab")), P("vocab", None)),
        check_vma=False,
    )
```

```python
import functools

import jax
import jax.numpy as jnp
from jax import lax
from jax.experimental import pallas as pl
from jax.experimental.pallas import tpu as pltpu
from jax.sharding import PartitionSpec as P

MESH = pl.DeviceIdType.MESH
STRIPE = 384


def plan_of(replicas, groups, stripes):
    tasks = [("hand", 2), ("line", 0), ("hand", 1)] + [("hand", offset) for offset in range(3, replicas)]
    tasks += [("line", 1), ("spread", 1), ("spread", 2), ("spread", 0)]
    tasks += [("spread", turn) for turn in range(3, groups)]
    tasks += [("first", 0), ("later", 0), ("first", 1), ("first", 2), ("line", 2), ("later", 1), ("later", 2)]
    for turn in range(3, groups):
        tasks += [("later", turn - 1)] * (turn > 3) + [("line", turn), ("first", turn)]
    tasks += [("logits", stripe) for stripe in range(stripes)]
    return tasks + [("stats", 0), ("later", groups - 1)]


def exchange(
    replicas, ranks, tokens, hidden, old, new, pieces, logprob,
    gathered, weight, logits, stats, relay, local_sem, weight_sem,
    line_send, line_recv, pair_send, pair_recv, relay_send, relay_recv,
    spread_send, spread_recv, cube_send, cube_recv, stat_send, stat_recv,
):
    d = lax.axis_index("dp")
    v = lax.axis_index("vocab")
    owners = ranks // replicas
    groups = ranks // 2
    g, core = v // 2, v % 2
    own_rows = hidden.shape[0]
    vocab_rows = old.shape[0]
    part = vocab_rows // replicas
    half = (part // 2) // 16 * 16
    bits = replicas.bit_length() - 1

    def remote(src, dst, send, recv, device):
        return pltpu.make_async_remote_copy(
            src_ref=src, dst_ref=dst, send_sem=send, recv_sem=recv, device_id=device, device_id_type=MESH
        )

    def rows_of(rank):
        return gathered.at[pl.ds(pl.multiple_of(rank * own_rows, own_rows), own_rows), :]

    def line(group, step, source=None):
        slot = rows_of(2 * group + core)
        way = 0 if step > 0 else 1
        return remote(
            slot if source is None else source, slot, line_send.at[way, group], line_recv.at[way, group],
            (d, v + 2 * step),
        )

    def pair(group, source=None):
        slot = rows_of(2 * group + core)
        return remote(
            slot if source is None else source, slot, pair_send.at[group], pair_recv.at[group], (d, v + 1 - 2 * core)
        )

    def pair_arrival(group):
        slot = rows_of(2 * group + 1 - core)
        return remote(slot, slot, pair_send.at[group], pair_recv.at[group], (d, v + 1 - 2 * core))

    ready = pltpu.get_barrier_semaphore()
    for offset in range(1, replicas):
        pl.semaphore_signal(ready, inc=1, device_id=(d ^ offset, v), device_id_type=MESH)
    for offset in range(1, ranks):
        pl.semaphore_signal(ready, inc=1, device_id=(d, (v + offset) % ranks), device_id_type=MESH)

    own_copy = pltpu.make_async_copy(hidden, rows_of(v), local_sem.at[0])
    weight_copy = pltpu.make_async_copy(old, weight, weight_sem.at[0])

    def line_start():
        pl.when(g < groups - 1)(lambda: line(g, 1, hidden).start())
        pl.when(g > 0)(lambda: line(g, -1, hidden).start())
        pair(g, hidden).start()

    def line_step(step):
        if step == 0:
            return line_start()

        def below():
            line(g - step, 1).wait_recv()
            pl.when(g < groups - 1)(lambda: line(g - step, 1).start())
            pair(g - step).start()

        def above():
            line(g + step, -1).wait_recv()
            pl.when(g > 0)(lambda: line(g + step, -1).start())
            pair(g + step).start()

        pl.when(g >= step)(below)
        pl.when(g + step < groups)(above)

    def hand(offset, owner):
        target = d ^ offset
        source = new.at[pl.ds(pl.multiple_of(owner * vocab_rows + target * part, 16), part), :]
        slot = relay.at[offset - 1, owner]
        index = (offset - 1) * owners + owner
        return remote(source, slot, relay_send.at[index], relay_recv.at[index], (target, v))

    def spread(turn, owner, source, stay=False):
        slot = pieces.at[v, pl.ds(pl.multiple_of(d * part, 16), part), :]
        if stay:
            return pltpu.make_async_copy(source, slot, spread_recv.at[v])
        rank = (g ^ turn) * owners + owner
        return remote(source, slot, spread_send.at[turn * owners + owner], spread_recv.at[v], (d, rank))

    def spread_from(turn, owner, source):
        if turn:
            return spread(turn, owner, source).start()
        pl.when(owner == core)(lambda: spread(turn, owner, source, stay=True).start())
        pl.when(owner != core)(lambda: spread(turn, owner, source).start())

    def in_turn():
        return [lax.rem(core + k, owners) for k in range(owners)]

    def spread_turn(turn):
        offset = d ^ g ^ turn

        def own():
            for owner in in_turn():
                first = pl.multiple_of(owner * vocab_rows + d * part, 16)
                spread_from(turn, owner, new.at[pl.ds(first, part), :])

        def handed():
            for owner in in_turn():
                hand(offset, owner).wait_recv()
                spread_from(turn, owner, relay.at[offset - 1, owner])

        pl.when(offset == 0)(own)
        pl.when(offset != 0)(handed)

    def spread_sent(turn, owner):
        def sent():
            spread(turn, owner, relay.at[0, owner]).wait_send()

        if turn:
            sent()
        else:
            pl.when(owner != core)(sent)

    def spread_arrival(source):
        slot = pieces.at[source, pl.ds(pl.multiple_of(d * part, 16), part), :]
        pltpu.make_async_copy(slot, slot, spread_recv.at[source]).wait()

    def span(holder, which):
        first, length = {"all": (0, part), "low": (0, half), "high": (half, part - half)}[which]
        return pl.ds(pl.multiple_of(holder * part + first, 16), length)

    links = []
    for mask in range(replicas):
        for bit in range(bits):
            if mask >> bit & 1:
                continue
            if mask == 0:
                links.append((mask, bit, "all"))
                continue
            if bit > mask.bit_length() - 1:
                links.append((mask, bit, "low"))
            if bit < (mask & -mask).bit_length() - 1:
                links.append((mask, bit, "high"))

    def cube(source, index):
        mask, bit, which = links[index]
        slot = pieces.at[source, span(d ^ mask, which), :]
        return remote(slot, slot, cube_send.at[source, index], cube_recv.at[source, index], (d ^ (1 << bit), v))

    def cube_arrival(source, index):
        mask, bit, which = links[index]
        slot = pieces.at[source, span(d ^ mask ^ (1 << bit), which), :]
        remote(slot, slot, cube_send.at[source, index], cube_recv.at[source, index], (d ^ (1 << bit), v)).wait_recv()

    def cube_level(source, level):
        for index, (mask, bit, which) in enumerate(links):
            if mask.bit_count() == level - 1:
                cube_arrival(source, index)
                for onward, (held, _, wanted) in enumerate(links):
                    if held == mask | 1 << bit and which in ("all", wanted):
                        cube(source, onward).start()

    def sources(turn):
        return [2 * (g ^ turn) + core, 2 * (g ^ turn) + 1 - core]

    def first_level(step):
        for source in sources(step):
            spread_arrival(source)
            for index, (mask, _, _) in enumerate(links):
                if mask == 0:
                    cube(source, index).start()

    def later_levels(step):
        for level in range(1, bits):
            for source in sources(step):
                cube_level(source, level)

    def logits_stripe(index):
        count = gathered.shape[0]
        if index == 0:
            for group in range(groups):
                pair_arrival(group).wait_recv()
            own_copy.wait()
            weight_copy.wait()
            floor = jnp.full((1, count), -jnp.inf, jnp.float32)
            stats[v] = jnp.concatenate([floor, jnp.zeros((7, count), jnp.float32)], axis=0)
        first = index * STRIPE
        logits[...] = lax.dot_general(
            weight[pl.ds(first, STRIPE), :], gathered[...], (((1,), (1,)), ((), ())),
            preferred_element_type=jnp.float32,
        )
        values = logits[...]
        top = stats[v, 0:1, :]
        higher = jnp.maximum(top, jnp.max(values, axis=0, keepdims=True))
        total = stats[v, 1:2, :] * jnp.exp(top - higher)
        total += jnp.sum(jnp.exp(values - higher), axis=0, keepdims=True)
        ids = lax.broadcasted_iota(jnp.int32, values.shape, 0) + (first + v * vocab_rows)
        target = jnp.sum(jnp.where(ids == tokens[...], values, 0.0), axis=0, keepdims=True)
        stats[v, 0:1, :] = higher
        stats[v, 1:2, :] = total
        stats[v, 2:3, :] += target

    def stat(offset):
        return remote(
            stats.at[v], stats.at[v], stat_send.at[offset], stat_recv.at[offset], (d, (v + offset) % ranks)
        )

    def stat_arrival(offset):
        source = (v + ranks - offset) % ranks
        remote(
            stats.at[source], stats.at[source], stat_send.at[offset], stat_recv.at[offset], (d, source)
        ).wait_recv()

    def hand_start(offset):
        for owner in in_turn():
            hand(offset, owner).start()

    def stats_start(_):
        for offset in range(1, ranks):
            stat(offset).start()

    run = {
        "hand": hand_start, "line": line_step, "spread": spread_turn, "first": first_level,
        "later": later_levels, "logits": logits_stripe, "stats": stats_start,
    }
    own_copy.start()
    weight_copy.start()
    pl.semaphore_wait(ready, replicas + ranks - 2)
    for task, index in plan_of(replicas, groups, vocab_rows // STRIPE):
        run[task](index)
    for source in range(ranks):
        cube_level(source, bits)
    for offset in range(1, ranks):
        stat_arrival(offset)
    top = stats[0, 0:1, :]
    for rank in range(1, ranks):
        top = jnp.maximum(top, stats[rank, 0:1, :])
    total = jnp.zeros_like(top)
    target = jnp.zeros_like(top)
    for rank in range(ranks):
        total += stats[rank, 1:2, :] * jnp.exp(stats[rank, 0:1, :] - top)
        target += stats[rank, 2:3, :]
    result = target - top - jnp.log(total)
    for rank in range(ranks):
        own = result[:, rank * own_rows : (rank + 1) * own_rows]
        pl.when(v == rank)(lambda: logprob.__setitem__((slice(0, 1), slice(0, own_rows)), own))

    for offset in range(1, ranks):
        stat(offset).wait_send()
    for owner in range(owners):
        for turn in range(groups):
            spread_sent(turn, owner)
        for offset in range(1, replicas):
            hand(offset, owner).wait_send()
    for source in range(ranks):
        for index in range(len(links)):
            cube(source, index).wait_send()
    for group in range(groups):
        pl.when((group <= g) & (g < groups - 1))(lambda: line(group, 1).wait_send())
        pl.when((group >= g) & (g > 0))(lambda: line(group, -1).wait_send())
        pair(group).wait_send()


def assemble(pieces, result, whole, logprob, sem):
    cols = pieces.shape[2]
    copies = [
        pltpu.make_async_copy(pieces.at[source], whole.at[:, pl.ds(source * cols, cols)], sem.at[source])
        for source in range(pieces.shape[0])
    ]
    for copy in copies:
        copy.start()
    logprob[...] = result[...]
    for copy in copies:
        copy.wait()


def on_device(hidden, tokens, old_weight, new_weight):
    ranks = lax.axis_size("vocab")
    replicas = lax.axis_size("dp")
    own_rows, width = hidden.shape
    vocab_rows = old_weight.shape[0]
    cols = new_weight.shape[1]
    count = own_rows * ranks
    dtype = new_weight.dtype
    groups = ranks // 2
    owners = ranks // replicas
    assert groups == replicas == 1 << (replicas.bit_length() - 1)
    bits = replicas.bit_length() - 1
    copies = sum(1 if mask == 0 else int(bit > mask.bit_length() - 1) + int(bit < (mask & -mask).bit_length() - 1)
                 for mask in range(replicas) for bit in range(bits) if not mask >> bit & 1)
    dma = pltpu.SemaphoreType.DMA
    anywhere = pl.BlockSpec(memory_space=pl.ANY)
    local = pl.BlockSpec(memory_space=pltpu.VMEM)
    pieces, logprob = pl.pallas_call(
        functools.partial(exchange, replicas, ranks),
        out_shape=(
            pltpu.VMEM((ranks, vocab_rows, cols), dtype),
            pltpu.VMEM((1, own_rows), jnp.float32),
        ),
        in_specs=[local, anywhere, anywhere, anywhere],
        out_specs=(local, local),
        scratch_shapes=[
            pltpu.VMEM((count, width), hidden.dtype),
            pltpu.VMEM((vocab_rows, width), old_weight.dtype),
            pltpu.VMEM((STRIPE, count), jnp.float32),
            pltpu.VMEM((ranks, 8, count), jnp.float32),
            pltpu.VMEM((replicas - 1, owners, vocab_rows // replicas, cols), dtype),
            dma((1,)), dma((1,)),
            dma((2, groups)), dma((2, groups)), dma((groups,)), dma((groups,)),
            dma(((replicas - 1) * owners,)), dma(((replicas - 1) * owners,)),
            dma((groups * owners,)), dma((ranks,)),
            dma((ranks, copies)), dma((ranks, copies)),
            dma((ranks,)), dma((ranks,)),
        ],
        compiler_params=pltpu.CompilerParams(
            collective_id=0, has_side_effects=True, vmem_limit_bytes=44 * 1024 * 1024
        ),
        name="exchange",
    )(tokens.reshape(1, count), hidden, old_weight, new_weight)
    if cols % 128 == 0:
        engine_weight, logprob = pl.pallas_call(
            assemble,
            out_shape=(
                jax.ShapeDtypeStruct((vocab_rows, ranks * cols), dtype),
                jax.ShapeDtypeStruct((1, own_rows), jnp.float32),
            ),
            in_specs=[anywhere, local],
            out_specs=(anywhere, local),
            scratch_shapes=[dma((ranks,))],
            compiler_params=pltpu.CompilerParams(vmem_limit_bytes=1024 * 1024),
            name="assemble",
        )(pieces, logprob)
    else:
        engine_weight = jnp.swapaxes(pieces, 0, 1).reshape(vocab_rows, ranks * cols)
    return (logprob.reshape(own_rows), engine_weight)


def solution(mesh):
    return jax.shard_map(
        on_device,
        mesh=mesh,
        in_specs=(P(("dp", "vocab"), None), P("dp"), P("vocab", None), P("dp", "vocab")),
        out_specs=(P(("dp", "vocab")), P("vocab", None)),
        check_vma=False,
    )
```
